256 devices in a mesh: freq: 8 (over y, core), tcol: 32 (over z, x).
Axes of the slice: x: 4, y: 4, z: 8, core: 2. Of those that a mesh axis runs over, the one named last changes fastest.
Arguments:
- data: bfloat16 [8, 2, 16384, 128], P('freq', None, 'tcol'), may hold values from -6 to 6
- left_factor: bfloat16 [8, 2, 16384, 1024], P('freq', None, 'tcol'), may hold values from -0.125 to 0.125
- right_factor: bfloat16 [8, 2, 16384, 1024], P('freq', None, 'tcol'), may hold values from -0.1875 to 0.1875
- ranks: int32 [8, 32, 32], P('freq'), may hold values from 1 to 32
- freq_index: int32 [8], P('freq'), may hold values from 0 to 229
Outputs:
- wavefield: float32 [8, 2, 16384, 128], P('freq', None, 'tcol')
- residual: float32 [8, 2, 16384, 128], P('freq', None, 'tcol')
The draws below stay inside these ranges and needn't reach their ends.
Inputs may be any that keep to these rules, and one draw needn't show every extreme that they name: `ranks`: the rank of each tile; factor columns at or beyond it are not part of the kernel.
All inputs are finite; a program needn't handle non-finite values.
Results may differ from the reference program's by a relative error of at most 0.006.
Values may be sent and summed in bfloat16 or wider, within the bound.
A program may use at most 64 MiB of HBM per device.

```python
import jax
import jax.numpy as jnp

TILE = 512
RANK = 32
SOURCES = 128
ITERS = 3
NTILES = 32
ORDER = 16384
FREQS = 8


def with_ends(drawn, key, low, top_value):
    place = [jax.random.randint(jax.random.fold_in(key, axis), (), 0, length) for axis, length in enumerate(drawn.shape)]
    main_axis = drawn.shape.index(max(drawn.shape))
    beside = place[:main_axis] + [(place[main_axis] + 1) % drawn.shape[main_axis]] + place[main_axis + 1:]
    return drawn.at[tuple(place)].set(low).at[tuple(beside)].set(top_value)


def block_scale(key, dims, cuts, least, largest):
    def one(position, parts):
        draws = jax.random.uniform(jax.random.fold_in(jax.random.fold_in(key, 6), position), (parts,), jnp.float32, least / len(cuts), largest / len(cuts))
        return jnp.repeat(jnp.exp(draws), dims[position] // parts).reshape((-1,) + (1,) * (len(dims) - position - 1))

    gain = one(*cuts[0])
    for cut in cuts[1:]:
        gain = gain * one(*cut)
    return gain


def gaussian(own_key, dims, spread, most, cuts=(), kind=jnp.bfloat16):
    result = jax.random.normal(own_key, dims, jnp.float32) * spread
    if len(cuts) > 0:
        result = block_scale(own_key, dims, cuts, -0.22, 0.18) * result
    return jnp.clip(result, min=-most, max=most).astype(kind)


def setup_inputs(seed: int = 0) -> dict:
    key_of = jax.random.split(jax.random.key(seed), 6)
    data = gaussian(key_of[0], (FREQS, 2, ORDER, SOURCES), 1.0, 6.0, ((0, 8), (2, 32)))
    left_factor = gaussian(key_of[1], (FREQS, 2, ORDER, NTILES * RANK), (2 * RANK * NTILES) ** -0.5, 0.125, ((0, 8), (2, 32)))
    right_factor = gaussian(key_of[2], (FREQS, 2, ORDER, NTILES * RANK), (2 * TILE) ** -0.5, 0.1875, ((0, 8), (2, 32)))
    ranks = with_ends(jax.random.randint(key_of[3], (FREQS, NTILES, NTILES), 1, RANK + 1), jax.random.fold_in(key_of[3], 1), 1, RANK).astype(jnp.int32)
    freq_index = with_ends(jax.random.randint(key_of[4], (FREQS,), 0, 230), jax.random.fold_in(key_of[4], 1), 0, 229).astype(jnp.int32)
    return {"data": data, "left_factor": left_factor, "right_factor": right_factor, "ranks": ranks, "freq_index": freq_index}


def tile_masks(ranks):
    return (jnp.arange(RANK)[None, None, None, :] < ranks[..., None]).astype(jnp.float32)


def apply_forward(left, right, field, masks):
    nfreq = field.shape[0]
    ntile = NTILES
    g = field.astype(jnp.bfloat16).astype(jnp.float32).reshape(nfreq, 2, ntile, TILE, field.shape[3])
    v = right.astype(jnp.float32).reshape(nfreq, 2, ntile, TILE, ntile * RANK)
    real = jnp.einsum('fjbq,fjbs->fjqs', v[:, 0], g[:, 0]) + jnp.einsum('fjbq,fjbs->fjqs', v[:, 1], g[:, 1])
    imag = jnp.einsum('fjbq,fjbs->fjqs', v[:, 0], g[:, 1]) - jnp.einsum('fjbq,fjbs->fjqs', v[:, 1], g[:, 0])
    colmask = jnp.transpose(masks, (0, 2, 1, 3)).reshape(nfreq, ntile, ntile * RANK)
    coeff = jnp.stack([real, imag], 1) * colmask[:, None, :, :, None]
    coeff = coeff.astype(jnp.bfloat16).astype(jnp.float32)
    coeff = coeff.reshape(nfreq, 2, ntile, ntile, RANK, -1)
    coeff = jnp.transpose(coeff, (0, 1, 3, 2, 4, 5)).reshape(nfreq, 2, ntile, ntile * RANK, -1)
    u = left.astype(jnp.float32).reshape(nfreq, 2, ntile, TILE, ntile * RANK)
    wreal = jnp.einsum('fiaq,fiqs->fias', u[:, 0], coeff[:, 0]) - jnp.einsum('fiaq,fiqs->fias', u[:, 1], coeff[:, 1])
    wimag = jnp.einsum('fiaq,fiqs->fias', u[:, 0], coeff[:, 1]) + jnp.einsum('fiaq,fiqs->fias', u[:, 1], coeff[:, 0])
    return jnp.stack([wreal, wimag], 1).reshape(field.shape)


def apply_adjoint(left, right, field, masks):
    nfreq = field.shape[0]
    ntile = NTILES
    r = field.astype(jnp.bfloat16).astype(jnp.float32).reshape(nfreq, 2, ntile, TILE, field.shape[3])
    u = left.astype(jnp.float32).reshape(nfreq, 2, ntile, TILE, ntile * RANK)
    real = jnp.einsum('fiaq,fias->fiqs', u[:, 0], r[:, 0]) + jnp.einsum('fiaq,fias->fiqs', u[:, 1], r[:, 1])
    imag = jnp.einsum('fiaq,fias->fiqs', u[:, 0], r[:, 1]) - jnp.einsum('fiaq,fias->fiqs', u[:, 1], r[:, 0])
    rowmask = masks.reshape(nfreq, ntile, ntile * RANK)
    back = jnp.stack([real, imag], 1) * rowmask[:, None, :, :, None]
    back = back.astype(jnp.bfloat16).astype(jnp.float32)
    back = back.reshape(nfreq, 2, ntile, ntile, RANK, -1)
    back = jnp.transpose(back, (0, 1, 3, 2, 4, 5)).reshape(nfreq, 2, ntile, ntile * RANK, -1)
    v = right.astype(jnp.float32).reshape(nfreq, 2, ntile, TILE, ntile * RANK)
    greal = jnp.einsum('fjbq,fjqs->fjbs', v[:, 0], back[:, 0]) - jnp.einsum('fjbq,fjqs->fjbs', v[:, 1], back[:, 1])
    gimag = jnp.einsum('fjbq,fjqs->fjbs', v[:, 0], back[:, 1]) + jnp.einsum('fjbq,fjqs->fjbs', v[:, 1], back[:, 0])
    return jnp.stack([greal, gimag], 1).reshape(field.shape)


def reference(data, left_factor, right_factor, ranks, freq_index):
    masks = tile_masks(ranks)
    damping = (0.1 + 0.9 * freq_index.astype(jnp.float32) / 229.0)[:, None, None, None]
    residual = data.astype(jnp.float32)
    wavefield = jnp.zeros_like(residual)
    direction = jnp.zeros_like(residual)
    image = jnp.zeros_like(residual)
    for step in range(ITERS):
        gradient = apply_adjoint(left_factor, right_factor, residual, masks) - damping * wavefield
        moved = apply_forward(left_factor, right_factor, gradient, masks)
        a11 = jnp.sum(moved * moved + damping * gradient * gradient, axis=(0, 1, 2))
        b1 = jnp.sum(moved * residual - damping * gradient * wavefield, axis=(0, 1, 2))
        if step == 0:
            alpha = b1 / (1.1 * a11)
            beta = jnp.zeros_like(alpha)
        else:
            a12 = jnp.sum(moved * image + damping * gradient * direction, axis=(0, 1, 2))
            a22 = jnp.sum(image * image + damping * direction * direction, axis=(0, 1, 2))
            b2 = jnp.sum(image * residual - damping * direction * wavefield, axis=(0, 1, 2))
            first = 1.1 * a11
            second = 1.1 * a22
            determinant = first * second - a12 * a12
            alpha = (b1 * second - a12 * b2) / determinant
            beta = (first * b2 - a12 * b1) / determinant
        direction = alpha * gradient + beta * direction
        image = alpha * moved + beta * image
        wavefield = wavefield + direction
        residual = residual - image
    return wavefield, residual
```

```python
import jax
import jax.numpy as jnp
from jax import lax
from jax.experimental import pallas as pl
from jax.experimental.pallas import tpu as pltpu
from jax.sharding import PartitionSpec as P

ITERS = 3
NX = 4
NZ = 8
NF = 8
RANK = 32
TILE = 512
HALF = 64
LANES = 128
BLOCK = NX * RANK
WIDE = NZ * BLOCK
ORDER = (4, 3, 5, 2, 6, 1, 7, 0)
PLACE = {dz: p for p, dz in enumerate(ORDER)}
GROUPS = 4
SPAN = NZ // GROUPS
DXS = (2, 1, 3, 0)
CHUNK = 64
MESH = pl.DeviceIdType.MESH
F32 = jnp.float32
BF16 = jnp.bfloat16


def kernel(
    data_hbm, left_hbm, right_hbm, ranks_ref, freq_ref,
    wave_out, resid_out,
    natural, turned, rawdata, spread, total, sendbuf, recvbuf,
    grad, ngrad, nump, direction, moved, image, wave, resid,
    zsrc, zslot, xsrc, xslot, fsrc, fslot,
    load_sem, bulk_send, bulk_recv, z_send, z_recv, x_send, x_recv, f_send, f_recv,
):
    f = lax.axis_index("freq")
    t = lax.axis_index("tcol")
    z = t // NX
    x = lax.rem(t, NX)

    def peer(dz, dx):
        return lax.rem(z + dz, NZ) * NX + lax.rem(x + dx, NX)

    barrier = pltpu.get_barrier_semaphore()
    for n in range(1, NZ * NX):
        pl.semaphore_signal(
            barrier, inc=1, device_id=(f, peer(n // NX, n % NX)), device_id_type=MESH
        )
    for df in range(1, NF):
        pl.semaphore_signal(
            barrier, inc=1, device_id=(lax.rem(f + df, NF), t), device_id_type=MESH
        )

    def load(factor, source, place):
        column = pl.multiple_of(lax.rem(z + ORDER[place], NZ) * BLOCK, BLOCK)
        return [
            pltpu.make_async_copy(
                source.at[0, c, :, pl.ds(column, BLOCK)],
                natural.at[factor, pl.ds(c * TILE, TILE), pl.ds(place * BLOCK, BLOCK)],
                load_sem.at[factor, place, c],
            )
            for c in range(2)
        ]

    data_copy = pltpu.make_async_copy(data_hbm.at[0], rawdata, load_sem.at[2, 0, 0])
    data_copy.start()
    for factor, source in ((0, left_hbm), (1, right_hbm)):
        for place in range(NZ):
            for copy in load(factor, source, place):
                copy.start()

    lane = lax.broadcasted_iota(jnp.int32, (1, LANES), 1)
    lower = lane < HALF
    sign = jnp.where(lower, 1.0, -1.0).astype(F32)
    damping = 0.1 + 0.9 * freq_ref[0].astype(F32) / 229.0

    def swap(value):
        return pltpu.roll(value, HALF, 1)

    def chunks(body, carry=None):
        def step(n, c):
            rows = pl.ds(pl.multiple_of(n * CHUNK, CHUNK), CHUNK)
            low = pl.ds(pl.multiple_of(n * CHUNK + TILE, CHUNK), CHUNK)
            return body(rows, low, c)

        return lax.fori_loop(0, TILE // CHUNK, step, carry)

    def put(rows, low, value):
        spread[rows, :] = value.astype(BF16)
        spread[low, :] = (swap(value) * sign).astype(BF16)

    def bulk(h, parity, place, dx):
        dz = ORDER[place]
        there = lax.rem(x + dx, NX)
        back = PLACE[(NZ - dz) % NZ]
        start = pl.multiple_of(place * BLOCK + there * RANK, RANK)
        land = pl.multiple_of(back * BLOCK + x * RANK, RANK)
        n = place * NX + dx
        return pltpu.make_async_remote_copy(
            src_ref=sendbuf.at[h, pl.ds(start, RANK), :],
            dst_ref=recvbuf.at[h, parity, pl.ds(land, RANK), :],
            send_sem=bulk_send.at[h, n],
            recv_sem=bulk_recv.at[h, parity, back * NX + dx],
            device_id=(f, peer(dz, dx)),
            device_id_type=MESH,
        )

    def arrival(h, parity, place, dx):
        there = lax.rem(x + NX - dx, NX)
        land = pl.multiple_of(place * BLOCK + there * RANK, RANK)
        return pltpu.make_async_remote_copy(
            src_ref=sendbuf.at[h, pl.ds(0, RANK), :],
            dst_ref=recvbuf.at[h, parity, pl.ds(land, RANK), :],
            send_sem=bulk_send.at[h, 0],
            recv_sem=bulk_recv.at[h, parity, place * NX + dx],
            device_id=(f, t),
            device_id_type=MESH,
        )

    def remote_pairs(places):
        return [(p, dx) for dx in DXS for p in places if not (ORDER[p] == 0 and dx == 0)]

    def drain(h, parity):
        for place, dx in remote_pairs(range(NZ)):
            bulk(h, parity, place, dx).wait_send()

    def contract(factor, h, parity, group):
        rows = pl.ds(group * SPAN * BLOCK, SPAN * BLOCK)
        coeff = jnp.dot(turned[factor, rows, :], spread[...], preferred_element_type=F32)
        sendbuf[h, rows, :] = coeff.astype(BF16)
        places = range(group * SPAN, (group + 1) * SPAN)
        if PLACE[0] in places:
            own = pl.ds(pl.multiple_of(PLACE[0] * BLOCK + x * RANK, RANK), RANK)
            recvbuf[h, parity, own, :] = sendbuf[h, own, :]
        for place, dx in remote_pairs(places):
            bulk(h, parity, place, dx).start()

    def expand(factor, h, parity):
        for group in range(GROUPS):
            for place, dx in remote_pairs(range(group * SPAN, (group + 1) * SPAN)):
                arrival(h, parity, place, dx).wait_recv()
            rows = pl.ds(group * SPAN * BLOCK, SPAN * BLOCK)
            part = jnp.dot(
                natural[factor, :, rows], recvbuf[h, parity, rows, :], preferred_element_type=F32
            )
            if group == 0:
                total[...] = part
            else:
                total[...] += part

    def expanded(rows, low):
        return total[rows, :] - swap(total[low, :]) * sign

    def zcopy(it, h, dz):
        return pltpu.make_async_remote_copy(
            src_ref=zsrc.at[it, h], dst_ref=zslot.at[it, h, dz - 1],
            send_sem=z_send.at[it, h, dz - 1], recv_sem=z_recv.at[it, h, dz - 1],
            device_id=(f, peer(dz, 0)), device_id_type=MESH,
        )

    def xcopy(it, h, dx):
        return pltpu.make_async_remote_copy(
            src_ref=xsrc.at[it, h], dst_ref=xslot.at[it, h, dx - 1],
            send_sem=x_send.at[it, h, dx - 1], recv_sem=x_recv.at[it, h, dx - 1],
            device_id=(f, peer(0, dx)), device_id_type=MESH,
        )

    def fcopy(it, h, df):
        return pltpu.make_async_remote_copy(
            src_ref=fsrc.at[it, h], dst_ref=fslot.at[it, h, df - 1],
            send_sem=f_send.at[it, h, df - 1], recv_sem=f_recv.at[it, h, df - 1],
            device_id=(lax.rem(f + df, NF), t), device_id_type=MESH,
        )

    def gathered(copy, slot, source, it, h, count):
        for d in range(1, count):
            copy(it, h, d).wait_recv()
        sums = source[it, h]
        for d in range(1, count):
            sums = sums + slot[it, h, d - 1]
        for d in range(1, count):
            copy(it, h, d).wait_send()
        return sums

    def z_to_x(it, h):
        xsrc[it, h] = gathered(zcopy, zslot, zsrc, it, h, NZ)
        for dx in range(1, NX):
            xcopy(it, h, dx).start()

    def x_to_f(it, h):
        fsrc[it, h] = gathered(xcopy, xslot, xsrc, it, h, NX)
        for df in range(1, NF):
            fcopy(it, h, df).start()

    def scales(it, h):
        sums = gathered(fcopy, fslot, fsrc, it, h, NF)
        a11, a12, a22, b1, b2 = [sums[n] + swap(sums[n]) for n in range(5)]
        if it == 0:
            return b1 / (1.1 * a11), None
        first = 1.1 * a11
        second = 1.1 * a22
        determinant = first * second - a12 * a12
        return (b1 * second - a12 * b2) / determinant, (first * b2 - a12 * b1) / determinant

    def inner(it, h):
        def fold(value):
            return jnp.sum(value.reshape(CHUNK // 8, 8, LANES), axis=0)

        def step(rows, low, sums):
            w = expanded(rows, low)
            moved[h, rows, :] = w
            if it < ITERS - 1:
                put(rows, low, w)
            g = grad[h, rows, :]
            r = resid[h, rows, :]
            dg = damping * g
            if it == 0:
                new = (w * w + dg * g, w * r)
            else:
                q = image[h, rows, :]
                p = direction[h, rows, :]
                v = wave[h, rows, :]
                dp = damping * p
                new = (w * w + dg * g, w * q + dg * p, q * q + dp * p, w * r - dg * v, q * r - dp * v)
            return tuple(s + fold(n) for s, n in zip(sums, new, strict=True))

        count = 2 if it == 0 else 5
        sums = chunks(step, tuple(jnp.zeros((8, LANES), F32) for _ in range(count)))
        sums = [jnp.sum(s, axis=0, keepdims=True) for s in sums]
        if it == 0:
            zero = jnp.zeros((1, LANES), F32)
            sums = [sums[0], zero, zero, sums[1], zero]
        for n in range(5):
            zsrc[it, h, n] = sums[n]
        for dz in (4, 3, 5, 2, 6, 1, 7):
            zcopy(it, h, dz).start()

    data_copy.wait()

    def begin(rows, low, carry):
        real = rawdata[0, rows, :].astype(F32)
        imag = rawdata[1, rows, :].astype(F32)
        resid[0, rows, :] = jnp.where(lower, real, swap(imag))
        resid[1, rows, :] = jnp.where(lower, swap(real), imag)
        return carry

    chunks(begin)

    def turn(factor, place):
        for copy in load(factor, left_hbm if factor == 0 else right_hbm, place):
            copy.wait()
        cols = pl.ds(place * BLOCK, BLOCK)
        if factor == 0:
            column = lax.rem(z + ORDER[place], NZ)
            limit = jnp.zeros((1, LANES), jnp.int32)
            for n in range(NX):
                limit = jnp.where(lane // RANK == n, ranks_ref[0, t, column * NX + n], limit)
            keep = lax.rem(lane, RANK) < limit
            keep = jnp.where(keep, 1.0, 0.0).astype(BF16)
        for n in range(2 * TILE // BLOCK):
            rows = pl.ds(n * BLOCK, BLOCK)
            tile = natural[factor, rows, cols]
            if factor == 0:
                tile = tile * keep
                natural[factor, rows, cols] = tile
            turned[factor, cols, rows] = tile.T

    def start_rows(rows, low, carry):
        put(rows, low, resid[0, rows, :])
        return carry

    chunks(start_rows)
    for group in range(GROUPS):
        for place in range(group * SPAN, (group + 1) * SPAN):
            turn(0, place)
        if group == 0:
            pl.semaphore_wait(barrier, NZ * NX - 1 + NF - 1)
        contract(0, 0, 0, group)

    def second_rows(rows, low, carry):
        put(rows, low, resid[1, rows, :])
        return carry

    chunks(second_rows)
    for group in range(GROUPS):
        contract(0, 1, 0, group)
    for place in range(NZ):
        turn(1, place)

    for it in range(ITERS):
        def adjoint(h, carry, it=it):
            expand(1, h, 0)
            drain(h, 0)
            if it == 0:
                def step(rows, low, c):
                    g = expanded(rows, low)
                    grad[h, rows, :] = g
                    put(rows, low, g)
                    return c

                chunks(step)
            else:
                @pl.when(h == 0)
                def _():
                    z_to_x(it - 1, 1)

                alpha, beta = scales(it - 1, h)

                def step(rows, low, c):
                    g = grad[h, rows, :]
                    n = alpha * (expanded(rows, low) + damping * g)
                    p = alpha * g
                    q = alpha * moved[h, rows, :]
                    if it == 1:
                        v = p
                    else:
                        n = n + beta * nump[h, rows, :]
                        p = p + beta * direction[h, rows, :]
                        q = q + beta * image[h, rows, :]
                        v = wave[h, rows, :] + p
                    g = g - n
                    put(rows, low, g)
                    grad[h, rows, :] = g
                    nump[h, rows, :] = n
                    direction[h, rows, :] = p
                    image[h, rows, :] = q
                    wave[h, rows, :] = v
                    resid[h, rows, :] = resid[h, rows, :] - q
                    return c

                chunks(step)
            for group in range(GROUPS):
                contract(1, h, 1, group)
            if it > 0:
                @pl.when(h == 0)
                def _():
                    x_to_f(it - 1, 1)
            return carry

        lax.fori_loop(0, 2, adjoint, 0)

        if it < ITERS - 1:
            def forward(h, carry, it=it):
                expand(0, h, 1)
                drain(h, 1)
                inner(it, h)
                for group in range(GROUPS):
                    contract(0, h, 0, group)
                return carry

            lax.fori_loop(0, 2, forward, 0)
            z_to_x(it, 0)
            x_to_f(it, 0)

    last = ITERS - 1

    def final(h, carry):
        expand(0, h, 1)
        drain(h, 1)
        inner(last, h)

        @pl.when(h == 0)
        def _():
            z_to_x(last, 0)

        return carry

    lax.fori_loop(0, 2, final, 0)

    def finish(h):
        alpha, beta = scales(last, h)

        def step(rows, low, c):
            p = alpha * grad[h, rows, :] + beta * direction[h, rows, :]
            q = alpha * moved[h, rows, :] + beta * image[h, rows, :]
            v = wave[h, rows, :] + p
            r = resid[h, rows, :] - q
            if h == 0:
                wave[h, rows, :] = v
                resid[h, rows, :] = r
            else:
                for out, mine, theirs in ((wave_out, wave, v), (resid_out, resid, r)):
                    other = mine[0, rows, :]
                    out[0, 0, rows, :] = jnp.where(lower, other, swap(theirs))
                    out[0, 1, rows, :] = jnp.where(lower, swap(other), theirs)
            return c

        chunks(step)

    x_to_f(last, 0)
    z_to_x(last, 1)
    finish(0)
    x_to_f(last, 1)
    finish(1)


def body(data, left_factor, right_factor, ranks, freq_index):
    anywhere = pl.BlockSpec(memory_space=pl.ANY)
    smem = pl.BlockSpec(memory_space=pltpu.SMEM)
    vmem = pl.BlockSpec(memory_space=pltpu.VMEM)
    field = pltpu.VMEM((2, TILE, LANES), F32)
    dma = pltpu.SemaphoreType.DMA
    out = jax.ShapeDtypeStruct((1, 2, TILE, LANES), F32)
    row = (5, 1, LANES)
    return pl.pallas_call(
        kernel,
        out_shape=(out, out),
        in_specs=[anywhere, anywhere, anywhere, smem, smem],
        out_specs=(vmem, vmem),
        scratch_shapes=[
            pltpu.VMEM((2, 2 * TILE, WIDE), BF16),
            pltpu.VMEM((2, WIDE, 2 * TILE), BF16),
            pltpu.VMEM((2, TILE, LANES), BF16),
            pltpu.VMEM((2 * TILE, LANES), BF16),
            pltpu.VMEM((2 * TILE, LANES), F32),
            pltpu.VMEM((2, WIDE, LANES), BF16),
            pltpu.VMEM((2, 2, WIDE, LANES), BF16),
            field, field, field, field, field, field, field, field,
            pltpu.VMEM((ITERS, 2) + row, F32),
            pltpu.VMEM((ITERS, 2, NZ - 1) + row, F32),
            pltpu.VMEM((ITERS, 2) + row, F32),
            pltpu.VMEM((ITERS, 2, NX - 1) + row, F32),
            pltpu.VMEM((ITERS, 2) + row, F32),
            pltpu.VMEM((ITERS, 2, NF - 1) + row, F32),
            dma((3, NZ, 2)),
            dma((2, NZ * NX)),
            dma((2, 2, NZ * NX)),
            dma((ITERS, 2, NZ - 1)),
            dma((ITERS, 2, NZ - 1)),
            dma((ITERS, 2, NX - 1)),
            dma((ITERS, 2, NX - 1)),
            dma((ITERS, 2, NF - 1)),
            dma((ITERS, 2, NF - 1)),
        ],
        compiler_params=pltpu.CompilerParams(
            collective_id=0, has_side_effects=True, vmem_limit_bytes=48 * 1024 * 1024
        ),
        name="tlr_descent",
    )(data, left_factor, right_factor, ranks, freq_index)


def solution(mesh):
    spec = P("freq", None, "tcol", None)
    return jax.shard_map(
        body,
        mesh=mesh,
        in_specs=(spec, spec, spec, P("freq", None, None), P("freq")),
        out_specs=(spec, spec),
        check_vma=False,
    )
```

```python
import jax
import jax.numpy as jnp
from jax import lax
from jax.experimental import pallas as pl
from jax.experimental.pallas import tpu as pltpu
from jax.sharding import PartitionSpec as P

ITERS = 3
NX = 4
NZ = 8
NF = 8
RANK = 32
TILE = 512
HALF = 64
LANES = 128
BLOCK = NX * RANK
WIDE = NZ * BLOCK
ORDER = (4, 3, 5, 2, 6, 1, 7, 0)
PLACE = {dz: p for p, dz in enumerate(ORDER)}
GROUPS = 4
PARTS = 2
SPAN = NZ // GROUPS
DXS = (2, 1, 3, 0)
CHUNK = 64
MESH = pl.DeviceIdType.MESH
F32 = jnp.float32
BF16 = jnp.bfloat16


def kernel(
    data_hbm, left_hbm, right_hbm, ranks_ref, freq_ref,
    wave_out, resid_out,
    natural, turned, rawdata, spread, total, sendbuf, recvbuf,
    grad, ngrad, nump, knump, direction, moved, image, wave, resid,
    zsrc, zslot, xsrc, xslot, fsrc, fslot, asrc, aslot,
    load_sem, bulk_send, bulk_recv, z_send, z_recv, x_send, x_recv, f_send, f_recv, a_send, a_recv,
):
    f = lax.axis_index("freq")
    t = lax.axis_index("tcol")
    z = t // NX
    x = lax.rem(t, NX)

    def peer(dz, dx):
        return lax.rem(z + dz, NZ) * NX + lax.rem(x + dx, NX)

    barrier = pltpu.get_barrier_semaphore()
    for n in range(1, NZ * NX):
        pl.semaphore_signal(
            barrier, inc=1, device_id=(f, peer(n // NX, n % NX)), device_id_type=MESH
        )
    for df in range(1, NF):
        pl.semaphore_signal(
            barrier, inc=1, device_id=(lax.rem(f + df, NF), t), device_id_type=MESH
        )

    def load(factor, source, place):
        column = pl.multiple_of(lax.rem(z + ORDER[place], NZ) * BLOCK, BLOCK)
        return [
            pltpu.make_async_copy(
                source.at[0, c, :, pl.ds(column, BLOCK)],
                natural.at[factor, pl.ds(c * TILE, TILE), pl.ds(place * BLOCK, BLOCK)],
                load_sem.at[factor, place, c],
            )
            for c in range(2)
        ]

    data_copy = pltpu.make_async_copy(data_hbm.at[0], rawdata, load_sem.at[2, 0, 0])
    data_copy.start()
    for factor, source in ((0, left_hbm), (1, right_hbm)):
        for place in range(NZ):
            for copy in load(factor, source, place):
                copy.start()

    lane = lax.broadcasted_iota(jnp.int32, (1, LANES), 1)
    lower = lane < HALF
    sign = jnp.where(lower, 1.0, -1.0).astype(F32)
    damping = 0.1 + 0.9 * freq_ref[0].astype(F32) / 229.0

    def swap(value):
        return pltpu.roll(value, HALF, 1)

    def chunks(body, carry=None):
        def step(n, c):
            rows = pl.ds(pl.multiple_of(n * CHUNK, CHUNK), CHUNK)
            low = pl.ds(pl.multiple_of(n * CHUNK + TILE, CHUNK), CHUNK)
            return body(rows, low, c)

        return lax.fori_loop(0, TILE // CHUNK, step, carry)

    def put(rows, low, value):
        spread[rows, :] = value.astype(BF16)
        spread[low, :] = (swap(value) * sign).astype(BF16)

    def bulk(h, parity, place, dx):
        dz = ORDER[place]
        there = lax.rem(x + dx, NX)
        back = PLACE[(NZ - dz) % NZ]
        start = pl.multiple_of(place * BLOCK + there * RANK, RANK)
        land = pl.multiple_of(back * BLOCK + x * RANK, RANK)
        n = place * NX + dx
        return pltpu.make_async_remote_copy(
            src_ref=sendbuf.at[h, parity, pl.ds(start, RANK), :],
            dst_ref=recvbuf.at[h, parity, pl.ds(land, RANK), :],
            send_sem=bulk_send.at[h, parity, n],
            recv_sem=bulk_recv.at[h, parity, back * NX + dx],
            device_id=(f, peer(dz, dx)),
            device_id_type=MESH,
        )

    def arrival(h, parity, place, dx):
        there = lax.rem(x + NX - dx, NX)
        land = pl.multiple_of(place * BLOCK + there * RANK, RANK)
        return pltpu.make_async_remote_copy(
            src_ref=sendbuf.at[h, parity, pl.ds(0, RANK), :],
            dst_ref=recvbuf.at[h, parity, pl.ds(land, RANK), :],
            send_sem=bulk_send.at[h, parity, 0],
            recv_sem=bulk_recv.at[h, parity, place * NX + dx],
            device_id=(f, t),
            device_id_type=MESH,
        )

    def remote_pairs(places):
        return [(p, dx) for dx in DXS for p in places if not (ORDER[p] == 0 and dx == 0)]

    def drain(h, parity):
        for place, dx in remote_pairs(range(NZ)):
            bulk(h, parity, place, dx).wait_send()

    def contract(factor, h, parity, group, groups):
        span = NZ // groups
        rows = pl.ds(group * span * BLOCK, span * BLOCK)
        coeff = jnp.dot(turned[factor, rows, :], spread[...], preferred_element_type=F32)
        sendbuf[h, parity, rows, :] = coeff.astype(BF16)
        places = range(group * span, (group + 1) * span)
        if PLACE[0] in places:
            own = pl.ds(pl.multiple_of(PLACE[0] * BLOCK + x * RANK, RANK), RANK)
            recvbuf[h, parity, own, :] = sendbuf[h, parity, own, :]
        for place, dx in remote_pairs(places):
            bulk(h, parity, place, dx).start()

    def expand(factor, h, parity):
        for group in range(GROUPS):
            for place, dx in remote_pairs(range(group * SPAN, (group + 1) * SPAN)):
                arrival(h, parity, place, dx).wait_recv()
            rows = pl.ds(group * SPAN * BLOCK, SPAN * BLOCK)
            part = jnp.dot(
                natural[factor, :, rows], recvbuf[h, parity, rows, :], preferred_element_type=F32
            )
            if group == 0:
                total[...] = part
            else:
                total[...] += part

    def expanded(rows, low):
        return total[rows, :] - swap(total[low, :]) * sign

    def zcopy(it, h, dz):
        return pltpu.make_async_remote_copy(
            src_ref=zsrc.at[it, h], dst_ref=zslot.at[it, h, dz - 1],
            send_sem=z_send.at[it, h, dz - 1], recv_sem=z_recv.at[it, h, dz - 1],
            device_id=(f, peer(dz, 0)), device_id_type=MESH,
        )

    def xcopy(it, h, dx):
        return pltpu.make_async_remote_copy(
            src_ref=xsrc.at[it, h], dst_ref=xslot.at[it, h, dx - 1],
            send_sem=x_send.at[it, h, dx - 1], recv_sem=x_recv.at[it, h, dx - 1],
            device_id=(f, peer(0, dx)), device_id_type=MESH,
        )

    def fcopy(it, h, df):
        return pltpu.make_async_remote_copy(
            src_ref=fsrc.at[it, h], dst_ref=fslot.at[it, h, df - 1],
            send_sem=f_send.at[it, h, df - 1], recv_sem=f_recv.at[it, h, df - 1],
            device_id=(lax.rem(f + df, NF), t), device_id_type=MESH,
        )

    def gathered(copy, slot, source, it, h, count):
        for d in range(1, count):
            copy(it, h, d).wait_recv()
        sums = source[it, h]
        for d in range(1, count):
            sums = sums + slot[it, h, d - 1]
        for d in range(1, count):
            copy(it, h, d).wait_send()
        return sums

    def acopy(h, dz, dx):
        n = dz * NX + dx - 1
        return pltpu.make_async_remote_copy(
            src_ref=asrc.at[h], dst_ref=aslot.at[h, n],
            send_sem=a_send.at[h, n], recv_sem=a_recv.at[h, n],
            device_id=(f, peer(dz, dx)), device_id_type=MESH,
        )

    def f_to_z(it, h):
        zsrc[it, h] = gathered(fcopy, fslot, fsrc, it, h, NF)
        for dz in (4, 3, 5, 2, 6, 1, 7):
            zcopy(it, h, dz).start()

    def z_to_x(it, h):
        xsrc[it, h] = gathered(zcopy, zslot, zsrc, it, h, NZ)
        for dx in range(1, NX):
            xcopy(it, h, dx).start()

    def f_to_all(it, h):
        asrc[h] = gathered(fcopy, fslot, fsrc, it, h, NF)
        for p, dx in remote_pairs(range(NZ)):
            acopy(h, ORDER[p], dx).start()

    def scales(it, h):
        if it < ITERS - 1:
            sums = gathered(xcopy, xslot, xsrc, it, h, NX)
        else:
            for p, dx in remote_pairs(range(NZ)):
                acopy(h, ORDER[p], dx).wait_recv()
            sums = asrc[h] + jnp.sum(aslot[h], axis=0)
            for p, dx in remote_pairs(range(NZ)):
                acopy(h, ORDER[p], dx).wait_send()
        packed = [sums[n] for n in range(3)]
        a11, a22, b2 = [jnp.where(lower, s, swap(s)) for s in packed]
        b1, a12 = [jnp.where(lower, swap(s), s) for s in packed[:2]]
        if it == 0:
            return b1 / (1.1 * a11), None
        first = 1.1 * a11
        second = 1.1 * a22
        determinant = first * second - a12 * a12
        return (b1 * second - a12 * b2) / determinant, (first * b2 - a12 * b1) / determinant

    def fold(value):
        return jnp.sum(value.reshape(CHUNK // 8, 8, LANES), axis=0)

    def announce(it, h, a11, b1, a22, a12, b2):
        sums = [jnp.sum(s, axis=0, keepdims=True) for s in (a11, b1, a22, a12, b2)]
        sums = [s + swap(s) for s in sums]
        fsrc[it, h, 0] = jnp.where(lower, sums[0], sums[1])
        fsrc[it, h, 1] = jnp.where(lower, sums[2], sums[3])
        fsrc[it, h, 2] = sums[4]
        for df in range(1, NF):
            fcopy(it, h, df).start()

    def blank(count):
        return tuple(jnp.zeros((8, LANES), F32) for _ in range(count))

    def add(sums, new):
        return tuple(s + fold(n) for s, n in zip(sums, new, strict=True))

    data_copy.wait()

    def begin(rows, low, carry):
        real = rawdata[0, rows, :].astype(F32)
        imag = rawdata[1, rows, :].astype(F32)
        resid[0, rows, :] = jnp.where(lower, real, swap(imag))
        resid[1, rows, :] = jnp.where(lower, swap(real), imag)
        return carry

    chunks(begin)

    def turn(factor, place):
        for copy in load(factor, left_hbm if factor == 0 else right_hbm, place):
            copy.wait()
        cols = pl.ds(place * BLOCK, BLOCK)
        if factor == 0:
            column = lax.rem(z + ORDER[place], NZ)
            limit = jnp.zeros((1, LANES), jnp.int32)
            for n in range(NX):
                limit = jnp.where(lane // RANK == n, ranks_ref[0, t, column * NX + n], limit)
            keep = lax.rem(lane, RANK) < limit
            keep = jnp.where(keep, 1.0, 0.0).astype(BF16)
        for n in range(2 * TILE // BLOCK):
            rows = pl.ds(n * BLOCK, BLOCK)
            tile = natural[factor, rows, cols]
            if factor == 0:
                tile = tile * keep
                natural[factor, rows, cols] = tile
            turned[factor, cols, rows] = tile.T

    def start_rows(rows, low, carry):
        put(rows, low, resid[0, rows, :])
        return carry

    chunks(start_rows)
    for group in range(GROUPS):
        for place in range(group * SPAN, (group + 1) * SPAN):
            turn(0, place)
        if group == 0:
            pl.semaphore_wait(barrier, NZ * NX - 1 + NF - 1)
        contract(0, 0, 0, group, GROUPS)

    def second_rows(rows, low, carry):
        put(rows, low, resid[1, rows, :])
        return carry

    chunks(second_rows)
    for group in range(PARTS):
        contract(0, 1, 0, group, PARTS)
    for place in range(NZ):
        turn(1, place)

    def first_adjoint(h, carry):
        expand(1, h, 0)

        def step(rows, low, c):
            g = expanded(rows, low)
            grad[h, rows, :] = g
            put(rows, low, g)
            return c

        chunks(step)
        for group in range(PARTS):
            contract(1, h, 1, group, PARTS)
        drain(h, 0)
        return carry

    def first_forward(h, carry):
        expand(0, h, 1)

        def step(rows, low, sums):
            w = expanded(rows, low)
            moved[h, rows, :] = w
            put(rows, low, w)
            g = grad[h, rows, :]
            return add(sums, (w * w + damping * g * g, w * resid[h, rows, :]))

        a11, b1 = chunks(step, blank(2))
        announce(0, h, a11, b1, *blank(3))

        @pl.when(h == 1)
        def _():
            f_to_z(0, 0)

        for group in range(PARTS):
            contract(0, h, 0, group, PARTS)
        drain(h, 1)
        return carry

    lax.fori_loop(0, 2, first_adjoint, 0)
    lax.fori_loop(0, 2, first_forward, 0)

    for it in range(ITERS - 1):
        def adjoint(h, carry, it=it):
            expand(1, h, 0)

            def step(rows, low, c):
                n = expanded(rows, low) + damping * grad[h, rows, :]
                ngrad[h, rows, :] = n
                put(rows, low, n)
                return c

            chunks(step)

            @pl.when(h == 0)
            def _():
                f_to_z(it, 1)

            @pl.when(h == 1)
            def _():
                z_to_x(it, 0)

            for group in range(PARTS):
                contract(1, h, 1, group, PARTS)
            drain(h, 0)

            @pl.when(h == 1)
            def _():
                z_to_x(it, 1)

            return carry

        def forward(h, carry, it=it):
            alpha, beta = scales(it, h)

            def update(rows, low, sums):
                g = grad[h, rows, :]
                n = alpha * ngrad[h, rows, :]
                p = alpha * g
                q = alpha * moved[h, rows, :]
                if it == 0:
                    v = p
                else:
                    n = n + beta * nump[h, rows, :]
                    p = p + beta * direction[h, rows, :]
                    q = q + beta * image[h, rows, :]
                    v = wave[h, rows, :] + p
                g = g - n
                r = resid[h, rows, :] - q
                grad[h, rows, :] = g
                nump[h, rows, :] = n
                direction[h, rows, :] = p
                image[h, rows, :] = q
                wave[h, rows, :] = v
                resid[h, rows, :] = r
                dg = damping * g
                dp = damping * p
                return add(sums, (dg * g, dg * p, q * q + dp * p, -dg * v, q * r - dp * v))

            sums = chunks(update, blank(5))
            expand(0, h, 1)

            def step(rows, low, sums):
                k = alpha * expanded(rows, low)
                if it > 0:
                    k = k + beta * knump[h, rows, :]
                w = moved[h, rows, :] - k
                moved[h, rows, :] = w
                if it < ITERS - 2:
                    knump[h, rows, :] = k
                    put(rows, low, w)
                return add(sums, (w * w, w * image[h, rows, :], w * resid[h, rows, :]))

            a11, a12, b1 = chunks(step, (sums[0], sums[1], sums[3]))
            announce(it + 1, h, a11, b1, sums[2], a12, sums[4])

            @pl.when(h == 1)
            def _():
                if it < ITERS - 2:
                    f_to_z(it + 1, 0)
                else:
                    f_to_all(it + 1, 0)

            if it < ITERS - 2:
                for group in range(PARTS):
                    contract(0, h, 0, group, PARTS)
            drain(h, 1)
            return carry

        lax.fori_loop(0, 2, adjoint, 0)
        lax.fori_loop(0, 2, forward, 0)

    last = ITERS - 1

    def finish(h):
        alpha, beta = scales(last, h)

        def step(rows, low, c):
            p = alpha * grad[h, rows, :] + beta * direction[h, rows, :]
            q = alpha * moved[h, rows, :] + beta * image[h, rows, :]
            v = wave[h, rows, :] + p
            r = resid[h, rows, :] - q
            if h == 0:
                wave[h, rows, :] = v
                resid[h, rows, :] = r
            else:
                for out, mine, theirs in ((wave_out, wave, v), (resid_out, resid, r)):
                    other = mine[0, rows, :]
                    out[0, 0, rows, :] = jnp.where(lower, other, swap(theirs))
                    out[0, 1, rows, :] = jnp.where(lower, swap(other), theirs)
            return c

        chunks(step)

    f_to_all(last, 1)
    finish(0)
    finish(1)


def relay(wave_in, resid_in, wave_out, resid_out, held, in_sem, out_sem):
    pieces = [(n, c) for n in range(2) for c in range(2)]
    sources, targets = (wave_in, resid_in), (wave_out, resid_out)
    loads = [
        pltpu.make_async_copy(sources[n].at[0, c], held.at[n, c], in_sem.at[n, c])
        for n, c in pieces
    ]
    stores = [
        pltpu.make_async_copy(held.at[n, c], targets[n].at[0, c], out_sem.at[n, c])
        for n, c in pieces
    ]
    for load in loads:
        load.start()
    for load, store in zip(loads, stores, strict=True):
        load.wait()
        store.start()
    for store in stores:
        store.wait()


def body(data, left_factor, right_factor, ranks, freq_index):
    anywhere = pl.BlockSpec(memory_space=pltpu.HBM)
    smem = pl.BlockSpec(memory_space=pltpu.SMEM)
    vmem = pl.BlockSpec(memory_space=pltpu.VMEM)
    field = pltpu.VMEM((2, TILE, LANES), F32)
    dma = pltpu.SemaphoreType.DMA
    out = jax.ShapeDtypeStruct((1, 2, TILE, LANES), F32)
    row = (3, 1, LANES)
    results = pl.pallas_call(
        kernel,
        out_shape=(out, out),
        in_specs=[anywhere, anywhere, anywhere, smem, smem],
        out_specs=(vmem, vmem),
        scratch_shapes=[
            pltpu.VMEM((2, 2 * TILE, WIDE), BF16),
            pltpu.VMEM((2, WIDE, 2 * TILE), BF16),
            pltpu.VMEM((2, TILE, LANES), BF16),
            pltpu.VMEM((2 * TILE, LANES), BF16),
            pltpu.VMEM((2 * TILE, LANES), F32),
            pltpu.VMEM((2, 2, WIDE, LANES), BF16),
            pltpu.VMEM((2, 2, WIDE, LANES), BF16),
            field, field, field, field, field, field, field, field, field,
            pltpu.VMEM((ITERS, 2) + row, F32),
            pltpu.VMEM((ITERS, 2, NZ - 1) + row, F32),
            pltpu.VMEM((ITERS, 2) + row, F32),
            pltpu.VMEM((ITERS, 2, NX - 1) + row, F32),
            pltpu.VMEM((ITERS, 2) + row, F32),
            pltpu.VMEM((ITERS, 2, NF - 1) + row, F32),
            pltpu.VMEM((2,) + row, F32),
            pltpu.VMEM((2, NZ * NX - 1) + row, F32),
            dma((3, NZ, 2)),
            dma((2, 2, NZ * NX)),
            dma((2, 2, NZ * NX)),
            dma((ITERS, 2, NZ - 1)),
            dma((ITERS, 2, NZ - 1)),
            dma((ITERS, 2, NX - 1)),
            dma((ITERS, 2, NX - 1)),
            dma((ITERS, 2, NF - 1)),
            dma((ITERS, 2, NF - 1)),
            dma((2, NZ * NX - 1)),
            dma((2, NZ * NX - 1)),
        ],
        compiler_params=pltpu.CompilerParams(
            collective_id=0, has_side_effects=True, vmem_limit_bytes=67043328
        ),
        name="tlr_descent",
    )(data, left_factor, right_factor, ranks, freq_index)
    return pl.pallas_call(
        relay,
        out_shape=(out, out),
        in_specs=[anywhere, anywhere],
        out_specs=(anywhere, anywhere),
        scratch_shapes=[pltpu.VMEM((2, 2, TILE, LANES), F32), dma((2, 2)), dma((2, 2))],
        name="relay",
    )(*results)


def solution(mesh):
    spec = P("freq", None, "tcol", None)
    return jax.shard_map(
        body,
        mesh=mesh,
        in_specs=(spec, spec, spec, P("freq", None, None), P("freq")),
        out_specs=(spec, spec),
        check_vma=False,
    )
```
